512 devices in a mesh: seq: 64 (over x, z), head: 8 (over y, core).
Axes of the slice: x: 4, y: 4, z: 16, core: 2. Of those that a mesh axis runs over, the one named last changes fastest.
Arguments:
- queries: bfloat16 [8192, 32, 128], P('seq', 'head'), may hold values from -6 to 6
- key_vectors: bfloat16 [8192, 32, 128], P('seq', 'head'), may hold values from -6 to 6
- values: bfloat16 [8192, 32, 128], P('seq', 'head'), may hold values from -6 to 6
- out_grad: bfloat16 [8192, 32, 128], P('seq', 'head'), may hold values from -6 to 6
- hidden_in: bfloat16 [8192, 2048], P('seq'), may hold values from -6 to 6
- decay_weight: bfloat16 [2048, 32], P(None, 'head'), may hold values from -0.125 to 0.125
- write_weight: bfloat16 [2048, 32], P(None, 'head'), may hold values from -0.125 to 0.125
- decay_bias: float32 [32], P('head'), may hold values from -2 to 2
- decay_log: float32 [32], P('head'), may hold values from -11 to -2
- write_bias: float32 [32], P('head'), may hold values from -9 to 0
- start_state: float32 [64, 32, 128, 128], P('seq', 'head'), may hold values from -4 to 4
Outputs:
- grad_queries: bfloat16 [8192, 32, 128], P('seq', 'head')
- grad_keys: bfloat16 [8192, 32, 128], P('seq', 'head')
- grad_values: bfloat16 [8192, 32, 128], P('seq', 'head')
- grad_hidden: bfloat16 [8192, 2048], P('seq', 'head')
- grad_decay_weight: float32 [2048, 32], P(None, 'head')
- grad_write_weight: float32 [2048, 32], P(None, 'head')
The draws below stay inside these ranges and needn't reach their ends.
All inputs are finite; a program needn't handle non-finite values.
Results may differ from the reference program's by a relative error of at most 0.014.
Values may be sent and summed in bfloat16 or wider, within the bound.
A program may use at most 64 MiB of HBM per device.

```python
from functools import partial
import jax
import jax.numpy as jnp
from jax import lax

D = 2048
HEADS = 32
DK = 128
DV = 128
TOK_DEV = 128
BLOCKS = 64
TOKENS = 8192


def block_scale(own_key, extent, shards, least, top_value):
    def one(axis_at, blocks):
        draws = jax.random.uniform(jax.random.fold_in(jax.random.fold_in(own_key, 6), axis_at), (blocks,), jnp.float32, least / len(shards), top_value / len(shards))
        return jnp.repeat(jnp.exp(draws), extent[axis_at] // blocks).reshape((-1,) + (1,) * (len(extent) - axis_at - 1))

    level = one(*shards[0])
    for cut in shards[1:]:
        level = level * one(*cut)
    return level


def scatter_about(own_key, extent, scale, most, split=(), held_as=jnp.bfloat16):
    loudness = block_scale(own_key, extent, split, -0.22, 0.18) if split else 1.0
    array = jax.random.normal(own_key, extent, jnp.float32) * scale * loudness
    return jnp.minimum(jnp.maximum(array, -most), most).astype(held_as)


def setup_inputs(seed: int = 0) -> dict:
    key_of = jax.random.split(jax.random.key(seed), 12)
    return {
        "queries": scatter_about(key_of[0], (TOKENS, HEADS, DK), 1.0, 6.0, ((0, 64), (1, 8))),
        "key_vectors": scatter_about(key_of[1], (TOKENS, HEADS, DK), 1.0, 6.0, ((0, 64), (1, 8))),
        "values": scatter_about(key_of[2], (TOKENS, HEADS, DV), 1.0, 6.0, ((0, 64), (1, 8))),
        "out_grad": scatter_about(key_of[3], (TOKENS, HEADS, DV), 1.0, 6.0, ((0, 64), (1, 8))),
        "hidden_in": scatter_about(key_of[4], (TOKENS, D), 1.0, 6.0, ((0, 64),)),
        "decay_weight": scatter_about(key_of[5], (D, HEADS), D ** -0.5, 0.125, ((1, 8),)),
        "write_weight": scatter_about(key_of[6], (D, HEADS), D ** -0.5, 0.125, ((1, 8),)),
        "decay_bias": jnp.clip(jax.random.uniform(key_of[7], (HEADS,), jnp.float32, -2.0, 2.0) * block_scale(key_of[7], (HEADS,), ((0, 8),), -0.4, 0.0), -2.0, 2.0),
        "decay_log": jnp.clip(-11.0 + 9.0 * jax.random.uniform(key_of[8], (HEADS,), jnp.float32) ** block_scale(key_of[8], (HEADS,), ((0, 8),), -0.2, 0.2), -11.0, -2.0),
        "write_bias": jnp.clip(-9.0 + 9.0 * jax.random.uniform(key_of[9], (HEADS,), jnp.float32) ** block_scale(key_of[9], (HEADS,), ((0, 8),), -0.2, 0.2), -9.0, 0.0),
        "start_state": scatter_about(key_of[10], (BLOCKS, HEADS, DK, DV), 0.5, 4.0, ((0, 64), (1, 8)), jnp.float32),
    }


EPSILON = 1e-06
PRECISION_MAXIMUM = lax.Precision.HIGHEST

def block_forward(decay_log, decay_bias, write_bias, queries, key_vectors, values, decay_logit, write_logit, initial_state):
    normalized_queries = queries * lax.rsqrt(lax.optimization_barrier(jnp.sum(queries * queries, axis=-1, keepdims=True)) + EPSILON)
    normalized_keys = key_vectors * lax.rsqrt(lax.optimization_barrier(jnp.sum(key_vectors * key_vectors, axis=-1, keepdims=True)) + EPSILON)
    write_rate = jax.nn.sigmoid(write_logit + write_bias)
    log_decay = -jnp.exp(decay_log) * jax.nn.softplus(decay_logit + decay_bias)
    log_prefix = jnp.cumsum(log_decay, axis=0).T
    block_size = queries.shape[0]
    positions = jnp.arange(block_size, dtype=jnp.int32)
    lower_mask = positions[:, None] >= positions[None, :]
    strict_mask = positions[:, None] > positions[None, :]
    log_gaps = jnp.where(lower_mask, log_prefix[:, :, None] - log_prefix[:, None, :], 0.0)
    decay_ratio = jnp.where(lower_mask, jnp.exp(log_gaps), 0.0)
    key_gram = jnp.einsum('ihk,jhk->hij', normalized_keys, normalized_keys, precision=PRECISION_MAXIMUM)
    coupling = jnp.where(strict_mask, write_rate.T[:, :, None] * decay_ratio * key_gram, 0.0)
    unit_lower = coupling + jnp.eye(block_size, dtype=coupling.dtype)
    cumulative_decay = jnp.exp(log_prefix)
    keys_against_state = jnp.einsum('dlu,lux->ldx', normalized_keys, initial_state, precision=PRECISION_MAXIMUM)
    right_side = write_rate.T[:, :, None] * (jnp.swapaxes(values, 0, 1) - cumulative_decay[:, :, None] * keys_against_state)
    value_updates = jax.scipy.linalg.solve_triangular(unit_lower, right_side, lower=True, unit_diagonal=True)
    query_keys = decay_ratio * jnp.einsum('ihk,jhk->hij', normalized_queries, normalized_keys, precision=PRECISION_MAXIMUM)
    layer_outputs = cumulative_decay[:, :, None] * jnp.einsum('dlu,lux->ldx', normalized_queries, initial_state, precision=PRECISION_MAXIMUM)
    layer_outputs = layer_outputs + jnp.einsum('hij,hjv->hiv', query_keys, value_updates, precision=PRECISION_MAXIMUM)
    final_decay_weights = decay_ratio[:, -1, :]
    final_state = cumulative_decay[:, -1][:, None, None] * initial_state + jnp.einsum('zg,gzi,zgq->ziq', final_decay_weights, normalized_keys, value_updates, precision=PRECISION_MAXIMUM)
    return (jnp.swapaxes(layer_outputs, 0, 1), final_state)

def reference(queries, key_vectors, values, out_grad, hidden_in, decay_weight, write_weight, decay_bias, decay_log, write_bias, start_state):
    decay_logit = jnp.dot(hidden_in.astype(jnp.float32), decay_weight.astype(jnp.float32), preferred_element_type=jnp.float32)
    write_logit = jnp.dot(hidden_in.astype(jnp.float32), write_weight.astype(jnp.float32), preferred_element_type=jnp.float32)
    head_count = queries.shape[1]

    def blocked(source):
        return source.astype(jnp.float32).reshape((BLOCKS, TOK_DEV) + source.shape[1:])
    inputs = (blocked(queries), blocked(key_vectors), blocked(values), blocked(out_grad), blocked(decay_logit), blocked(write_logit), start_state)
    forward = partial(block_forward, decay_log, decay_bias, write_bias)

    def backward_block(carried, pieces):
        query_rows, key_rows, value_rows, grad_rows, decay_rows, write_rows, initial_state = pieces
        primal, pullback = jax.vjp(forward, query_rows, key_rows, value_rows, decay_rows, write_rows, initial_state)
        gradients = pullback((grad_rows, carried))
        return (gradients[5], gradients[:5])
    carried_init = jnp.zeros((head_count, DK, DV), jnp.float32)
    _, gradients = lax.scan(backward_block, carried_init, inputs, reverse=True)

    def joined(source):
        return source.reshape((TOKENS,) + source.shape[2:])
    grad_queries = joined(gradients[0]).astype(jnp.bfloat16)
    grad_keys = joined(gradients[1]).astype(jnp.bfloat16)
    grad_values = joined(gradients[2]).astype(jnp.bfloat16)
    decay_grads = joined(gradients[3]).astype(jnp.bfloat16)
    write_grads = joined(gradients[4]).astype(jnp.bfloat16)
    grad_decay_weight = jnp.dot(hidden_in.T.astype(jnp.float32), decay_grads.astype(jnp.float32), preferred_element_type=jnp.float32)
    grad_write_weight = jnp.dot(hidden_in.T.astype(jnp.float32), write_grads.astype(jnp.float32), preferred_element_type=jnp.float32)
    grad_hidden = jnp.dot(decay_grads.astype(jnp.float32), decay_weight.T.astype(jnp.float32), preferred_element_type=jnp.float32) + jnp.dot(write_grads.astype(jnp.float32), write_weight.T.astype(jnp.float32), preferred_element_type=jnp.float32)
    return (grad_queries, grad_keys, grad_values, grad_hidden.astype(jnp.bfloat16), grad_decay_weight, grad_write_weight)
```

```python
import functools

import jax
import jax.numpy as jnp
from jax import lax
from jax.experimental import pallas as pl
from jax.experimental.pallas import tpu as pltpu
from jax.sharding import Mesh
from jax.sharding import PartitionSpec as P

F32 = jnp.float32
BF16 = jnp.bfloat16
EPSILON = 1e-06
NN = (((1,), (0,)), ((), ()))
NT = (((1,), (1,)), ((), ()))
TN = (((0,), (0,)), ((), ()))
MESH = pl.DeviceIdType.MESH


def mm(a, b, dims=NN):
    return lax.dot_general(
        a.astype(BF16), b.astype(BF16), dims, preferred_element_type=F32
    )


def halves(a):
    high = a.astype(BF16)
    return high, (a - high.astype(F32)).astype(BF16)


def mm3(a, b, dims=NN):
    ah, al = halves(a)
    bh, bl = halves(b)
    return mm(ah, bh, dims) + (mm(ah, bl, dims) + mm(al, bh, dims))


def mm_ones(a, ones, dims=NN):
    high, rest = halves(a)
    mid = (a - high.astype(F32) - rest.astype(F32)).astype(BF16)
    return mm(high, ones, dims) + (mm(rest, ones, dims) + mm(mid, ones, dims))


def position_masks(n):
    row = lax.broadcasted_iota(jnp.int32, (n, n), 0)
    col = lax.broadcasted_iota(jnp.int32, (n, n), 1)
    return row, col


def gate_rows(logits, decay_bias, decay_scale, write_bias, heads):
    shifted = logits[:heads] + decay_bias
    soft = jnp.maximum(shifted, 0.0) + jnp.log1p(jnp.exp(-jnp.abs(shifted)))
    log_decay = -decay_scale * soft
    n = logits.shape[1]
    row, col = position_masks(n)
    upper = jnp.where(row <= col, 1.0, 0.0).astype(BF16)
    prefix = mm_ones(log_decay, upper)
    written = 1.0 / (1.0 + jnp.exp(-(logits[heads:] + write_bias)))
    slope = -decay_scale / (1.0 + jnp.exp(-shifted))
    return prefix, written, slope


def unit(x):
    scale = lax.rsqrt(jnp.sum(x * x, axis=-1, keepdims=True) + EPSILON)
    return x * scale, scale


def lockstep(fn, *lists):
    return [fn(*items) for items in zip(*lists)]


def first_half(qs, ks, vs, dys, states, prefix_rows, prefix_cols, write_cols):
    n = qs[0].shape[0]
    row, col = position_masks(n)
    lower, strict = row >= col, row > col
    qn = lockstep(unit, qs)
    kn = lockstep(unit, ks)
    q_scale = [s for _, s in qn]
    k_scale = [s for _, s in kn]
    qn = [x for x, _ in qn]
    kn = [x for x, _ in kn]
    ratio = lockstep(
        lambda c, r: jnp.where(lower, jnp.exp(jnp.where(lower, c - r, 0.0)), 0.0),
        prefix_cols,
        prefix_rows,
    )
    gram = lockstep(lambda k: mm3(k, k, NT), kn)
    gram = lockstep(lambda r, g: jnp.where(strict, r * g, 0.0), ratio, gram)
    coupling = lockstep(lambda b, g: b * g, write_cols, gram)
    near = (row ^ col) == 1
    inverse = lockstep(
        lambda c: jnp.where(row == col, 1.0, 0.0) - jnp.where(near, c, 0.0), coupling
    )
    size = 2
    while size < n:
        joint = ((row ^ col) >= size) & ((row ^ col) < 2 * size)
        part = lockstep(
            lambda c, t: mm3(jnp.where(joint, c, 0.0), t), coupling, inverse
        )
        inverse = lockstep(lambda t, p: t - mm3(t, p), inverse, part)
        size *= 2
    gain = lockstep(jnp.exp, prefix_cols)
    last = [c[n - 1 : n] for c in prefix_cols]
    tail = lockstep(lambda l, c: jnp.exp(l - c), last, prefix_cols)
    keyed = lockstep(lambda b, g, k: b * g * k, write_cols, gain, kn)
    solved = lockstep(mm, inverse, keyed)
    tailed = lockstep(lambda w, k: w * k, tail, kn)
    map_a = lockstep(lambda x, w: -mm(x, w, TN), solved, tailed)
    scores = lockstep(lambda q, k, r: r * mm(q, k, NT), qn, kn, ratio)
    reach = lockstep(lambda g, q, p, x: g * q - mm(p, x), gain, qn, scores, solved)
    map_b = lockstep(lambda r, d: mm(r, d, TN), reach, dys)
    return dict(
        qn=qn, kn=kn, q_scale=q_scale, k_scale=k_scale, ratio=ratio, gram=gram,
        coupling=coupling, inverse=inverse, gain=gain, tail=tail, tailed=tailed,
        scores=scores, map_a=map_a, map_b=map_b,
    )


def between(vs, dys, states, write_cols, f):
    n = vs[0].shape[0]
    row, col = position_masks(n)
    lower = row >= col
    key_state = lockstep(mm, f["kn"], states)
    error = lockstep(lambda v, g, s: v - g * s, vs, f["gain"], key_state)
    updates = lockstep(lambda t, b, e: mm(t, b * e), f["inverse"], write_cols, error)
    pulled = lockstep(lambda p, d: mm(p, d, TN), f["scores"], dys)
    d_scores = lockstep(lambda d, u: jnp.where(lower, mm(d, u, NT), 0.0), dys, updates)
    d_qk = lockstep(lambda r, d: r * d, f["ratio"], d_scores)
    out_state = lockstep(lambda g, d, s: g * mm(d, s, NT), f["gain"], dys, states)
    d_qn = lockstep(lambda o, d, k: o + mm(d, k), out_state, d_qk, f["kn"])
    d_q = lockstep(
        lambda d, q, s: s * (d - q * jnp.sum(q * d, axis=-1, keepdims=True)),
        d_qn, f["qn"], f["q_scale"],
    )
    d_kn = lockstep(lambda d, q: mm(d, q, TN), d_qk, f["qn"])
    paired = lockstep(lambda d, p: d * p, d_scores, f["scores"])
    gain_q = lockstep(
        lambda o, q: jnp.sum(o * q, axis=-1, keepdims=True), out_state, f["qn"]
    )
    return dict(
        key_state=key_state, error=error, updates=updates, pulled=pulled, d_q=d_q,
        d_kn=d_kn, paired=paired, gain_q=gain_q,
    )


def second_half(states, write_cols, f, g, ends):
    n = states[0].shape[0]
    row, col = position_masks(n)
    strict = row > col
    d_updates = lockstep(lambda p, w, d: p + mm(w, d), g["pulled"], f["tailed"], ends)
    d_right = lockstep(lambda t, d: mm(t, d, TN), f["inverse"], d_updates)
    d_v = lockstep(lambda b, d: b * d, write_cols, d_right)
    d_couple = lockstep(
        lambda d, u: jnp.where(strict, -mm(d, u, NT), 0.0), d_right, g["updates"]
    )
    d_gram = lockstep(lambda b, r, d: b * r * d, write_cols, f["ratio"], d_couple)
    right_state = lockstep(
        lambda b, c, d, s: b * c * mm(d, s, NT), write_cols, f["gain"], d_right, states
    )
    tail_keys = lockstep(lambda w, u, d: w * mm(u, d, NT), f["tail"], g["updates"], ends)
    d_kn = lockstep(
        lambda a, r, t, m, k: a - r + t + (mm(m, k) + mm(m, k, TN)),
        g["d_kn"], right_state, tail_keys, d_gram, f["kn"],
    )
    d_k = lockstep(
        lambda d, k, s: s * (d - k * jnp.sum(k * d, axis=-1, keepdims=True)),
        d_kn, f["kn"], f["k_scale"],
    )
    d_write = lockstep(
        lambda d, e, m, c: jnp.sum(d * e + m * c, axis=-1, keepdims=True),
        d_right, g["error"], d_couple, f["gram"],
    )
    pairs = lockstep(lambda m, c, p: m * c + p, d_couple, f["coupling"], g["paired"])
    tail_sum = lockstep(
        lambda k, t: jnp.sum(k * t, axis=-1, keepdims=True), f["kn"], tail_keys
    )
    at_end = lax.broadcasted_iota(jnp.int32, (n, 1), 0) == n - 1
    d_prefix = lockstep(
        lambda p, q, b, c, d, s, t, st, e: jnp.sum(p, axis=-1, keepdims=True)
        + q
        - b * c * jnp.sum(d * s, axis=-1, keepdims=True)
        - t
        + jnp.where(
            at_end,
            jnp.sum(t, axis=0, keepdims=True)
            + c[n - 1 : n]
            * jnp.sum(jnp.sum(st * e, axis=-1, keepdims=True), axis=0, keepdims=True),
            0.0,
        ),
        pairs, g["gain_q"], write_cols, f["gain"], d_right, g["key_state"], tail_sum,
        states, ends,
    )
    d_prefix_row = lockstep(lambda p: jnp.sum(p, axis=0, keepdims=True), pairs)
    return d_v, d_k, d_write, d_prefix, d_prefix_row


def gate_grads(d_prefix, d_write, written, slope):
    n = d_prefix.shape[1]
    row, col = position_masks(n)
    later = jnp.where(row >= col, 1.0, 0.0).astype(BF16)
    d_decay_logit = mm_ones(d_prefix, later) * slope
    d_write_logit = d_write * written * (1.0 - written)
    return jnp.concatenate([d_decay_logit, d_write_logit], axis=0)


def join(map_a, map_b, own_decay, in_a, in_b, in_decay):
    wide = mm(map_a, jnp.concatenate([in_a, in_b], axis=1))
    n = in_a.shape[1]
    new_a = wide[:, :n] + own_decay * in_a.astype(F32) + in_decay * map_a.astype(F32)
    new_b = wide[:, n:] + own_decay * in_b.astype(F32) + map_b.astype(F32)
    return new_a, new_b


def applied(map_a, map_b, decay, x):
    return map_b.astype(F32) + decay * x.astype(F32) + mm(map_a, x)


def kernel(
    sizes, axes,
    q_ref, k_ref, v_ref, dy_ref, hid_ref, wd_ref, ww_ref, s0_ref,
    dbias_ref, dlog_ref, wbias_ref,
    gq_ref, gk_ref, gv_ref, gh_ref, gdw_ref, gww_ref,
    qs, ks, vs, ds, wt, wall, gall, glr, own_a, own_b,
    m1r, m1s, m2r, m2s, fr, fs, gr, pw, rsr, xs, xr, wf,
    w_sem, g_sem, gl_sem, m1_sem, m2_sem, f_sem, gr_sem, rs_sem, x_sem, wf_sem,
    w_out, g_out, gl_out, m1_out, m2_out, f_out, d_out, gr_out, rs_out, x_out, wf_out,
):
    nx, na, nb, nh = sizes
    nz = na * nb
    heads, n = s0_ref.shape[0], s0_ref.shape[1]
    rows = 2 * heads
    width = hid_ref.shape[1] // nh
    piece = hid_ref.shape[1] // nz
    x, z, h = (lax.axis_index(axis) for axis in axes)
    a, b = z // nb, z % nb
    every = list(range(heads))

    def put(src, dst, send, recv, at):
        return pltpu.make_async_remote_copy(
            src_ref=src, dst_ref=dst, send_sem=send, recv_sem=recv,
            device_id=at, device_id_type=MESH,
        )

    def z_peer(i):
        return lax.rem(z + i, nz)

    def x_peer(i):
        return lax.rem(x + i, nx)

    def h_peer(i):
        return lax.rem(h + i, nh)

    barrier = pltpu.get_barrier_semaphore()
    for i in range(1, nz):
        pl.semaphore_signal(
            barrier, inc=1, device_id=(x, z_peer(i), h), device_id_type=MESH
        )
    for i in range(1, nx):
        pl.semaphore_signal(
            barrier, inc=1, device_id=(x_peer(i), z, h), device_id_type=MESH
        )
    for i in range(1, nh):
        pl.semaphore_signal(
            barrier, inc=1, device_id=(x, z, h_peer(i)), device_id_type=MESH
        )

    qs[...] = q_ref[...].astype(F32)
    ks[...] = k_ref[...].astype(F32)
    vs[...] = v_ref[...].astype(F32)
    ds[...] = dy_ref[...].astype(F32)

    def head_rows(ref):
        return [ref[pl.ds(i, n, stride=heads), :] for i in every]

    q, k, v, dy = head_rows(qs), head_rows(ks), head_rows(vs), head_rows(ds)
    states = [s0_ref[i] for i in every]
    wt[...] = jnp.concatenate(
        [wd_ref[...].astype(F32), ww_ref[...].astype(F32)], axis=0
    ).astype(BF16)
    logits = mm(wt[...], hid_ref[...], NT)
    where = lax.broadcasted_iota(jnp.int32, (heads, n), 0)

    def spread(ref):
        out = jnp.full((heads, n), ref[0], F32)
        for i in every[1:]:
            out = jnp.where(where == i, ref[i], out)
        return out

    prefix, written, slope = gate_rows(
        logits, spread(dbias_ref), jnp.exp(spread(dlog_ref)), spread(wbias_ref), heads
    )
    both = jnp.concatenate([prefix, written], axis=0)
    glr[z] = both
    turned = both.T
    prefix_cols = [turned[:, i : i + 1] for i in every]
    write_cols = [turned[:, heads + i : heads + i + 1] for i in every]
    prefix_rows = [prefix[i : i + 1] for i in every]

    pl.semaphore_wait(barrier, (nz - 1) + (nx - 1) + (nh - 1))

    sent = []
    for i in range(1, nz):
        copy = put(
            glr.at[z], glr.at[z], gl_out.at[i], gl_sem.at[z], (x, z_peer(i), h)
        )
        copy.start()
        sent.append(copy)
    for i in range(1, nh):
        to = h_peer(i)
        copy = put(
            wt.at[:, pl.ds(pl.multiple_of(to * width, 128), width)],
            wall.at[h], w_out.at[i], w_sem.at[h], (x, z, to),
        )
        copy.start()
        sent.append(copy)
    wall[h] = wt[:, pl.ds(pl.multiple_of(h * width, 128), width)]

    f = first_half(q, k, v, dy, states, prefix_rows, prefix_cols, write_cols)
    for i in every:
        own_a[i] = f["map_a"][i]
        own_b[i] = f["map_b"][i]

    @pl.when(b == nb - 1)
    def _():
        m1r[...] = jnp.zeros_like(m1r)

    @pl.when(a == na - 1)
    def _():
        m2r[...] = jnp.zeros_like(m2r)

    @pl.when(x == nx - 1)
    def _():
        fr[...] = jnp.zeros_like(fr)

    for i in range(1, nz):
        put(
            glr.at[z], glr.at[z_peer(i)], gl_out.at[i], gl_sem.at[z_peer(i)], (x, z, h)
        ).wait_recv()

    in_group = jnp.zeros((rows, n), F32)
    in_line = jnp.zeros((rows, n), F32)
    for i in range(nz):
        tile = glr[i]
        in_group = in_group + jnp.where((i > z) & (i < (a + 1) * nb), tile, 0.0)
        in_line = in_line + jnp.where(i >= (a + 1) * nb, tile, 0.0)
    own_decay = jnp.exp(both)
    group_decay = jnp.exp(in_group)
    line_decay = jnp.exp(in_line)
    whole_decay = jnp.exp(both + in_group)
    full_decay = jnp.exp(both + in_group + in_line)

    def scalar(tile, i):
        return tile[i : i + 1, n - 1 : n]

    for i in every:
        @pl.when(b < nb - 1)
        def _():
            put(
                m1s.at[i], m1r.at[i], m1_out.at[i], m1_sem.at[i], (x, z, h)
            ).wait_recv()

        new_a, new_b = join(
            own_a[i], own_b[i], scalar(own_decay, i),
            m1r[i, 0], m1r[i, 1], scalar(group_decay, i),
        )
        m1s[i, 0] = new_a.astype(BF16)
        m1s[i, 1] = new_b.astype(BF16)

        @pl.when(b > 0)
        def _():
            put(
                m1s.at[i], m1r.at[i], m1_out.at[i], m1_sem.at[i], (x, z - 1, h)
            ).start()

        @pl.when(b == 0)
        def _():
            @pl.when(a < na - 1)
            def _():
                put(
                    m2s.at[i], m2r.at[i], m2_out.at[i], m2_sem.at[i], (x, z, h)
                ).wait_recv()

            line_a, line_b = join(
                m1s[i, 0], m1s[i, 1], scalar(whole_decay, i),
                m2r[i, 0], m2r[i, 1], scalar(line_decay, i),
            )
            m2s[i, 0] = line_a.astype(BF16)
            m2s[i, 1] = line_b.astype(BF16)

            @pl.when(a > 0)
            def _():
                put(
                    m2s.at[i], m2r.at[i], m2_out.at[i], m2_sem.at[i], (x, z - nb, h)
                ).start()

    @pl.when(b == 0)
    def _():
        for i in every:
            @pl.when((a > 0) | (x < nx - 1))
            def _():
                put(fs.at[i], fr.at[i], f_out.at[i], f_sem.at[i], (x, z, h)).wait_recv()

            @pl.when(a == 0)
            def _():
                @pl.when(x > 0)
                def _():
                    fs[i] = applied(
                        m2s[i, 0], m2s[i, 1], scalar(full_decay, i), fr[i]
                    ).astype(BF16)
                    put(
                        fs.at[i], fr.at[i], f_out.at[i], f_sem.at[i], (x - 1, z, h)
                    ).start()

                for j in range(1, na):
                    put(
                        fr.at[i], fr.at[i], d_out.at[i, j], f_sem.at[i], (x, j * nb, h)
                    ).start()

            gr[i] = applied(
                m2r[i, 0], m2r[i, 1], scalar(line_decay, i), fr[i]
            ).astype(BF16)
            for j in range(1, nb):
                put(
                    gr.at[i], gr.at[i], gr_out.at[i, j], gr_sem.at[i], (x, z + j, h)
                ).start()

    g = between(v, dy, states, write_cols, f)
    for i in every:
        gq_scratch = g["d_q"][i]
        qs[pl.ds(i, n, stride=heads), :] = gq_scratch
    gq_ref[...] = qs[...].astype(BF16)

    @pl.when(b > 0)
    def _():
        for i in every:
            put(gr.at[i], gr.at[i], gr_out.at[i, 1], gr_sem.at[i], (x, z, h)).wait_recv()

    ends = [
        applied(m1r[i, 0], m1r[i, 1], scalar(group_decay, i), gr[i]) for i in every
    ]
    d_v, d_k, d_write, d_prefix, d_prefix_row = second_half(
        states, write_cols, f, g, ends
    )
    columns = jnp.concatenate(d_prefix + d_write, axis=1).T
    grads = gate_grads(
        columns[:heads] - jnp.concatenate(d_prefix_row, axis=0),
        columns[heads:], written, slope,
    ).astype(BF16)
    gall[h] = grads
    for i in range(1, nh):
        copy = put(
            gall.at[h], gall.at[h], g_out.at[i], g_sem.at[h], (x, z, h_peer(i))
        )
        copy.start()
        sent.append(copy)
    for j in range(nz):
        pw[j] = mm(grads, hid_ref[:, j * piece : (j + 1) * piece]).astype(BF16)
    for i in range(1, nz):
        to = z_peer(i)
        copy = put(pw.at[to], rsr.at[z], rs_out.at[i], rs_sem.at[z], (x, to, h))
        copy.start()
        sent.append(copy)
    rsr[z] = pw[z]

    for i in every:
        ks[pl.ds(i, n, stride=heads), :] = d_k[i]
        vs[pl.ds(i, n, stride=heads), :] = d_v[i]
    gk_ref[...] = ks[...].astype(BF16)
    gv_ref[...] = vs[...].astype(BF16)

    for i in range(1, nh):
        put(
            wall.at[h], wall.at[h_peer(i)], w_out.at[i], w_sem.at[h_peer(i)], (x, z, h)
        ).wait_recv()
        put(
            gall.at[h], gall.at[h_peer(i)], g_out.at[i], g_sem.at[h_peer(i)], (x, z, h)
        ).wait_recv()
    total = jnp.zeros((n, width), F32)
    for i in range(nh):
        total = total + mm(gall[i], wall[i], TN)
    gh_ref[...] = total.astype(BF16)

    for i in range(1, nz):
        put(
            pw.at[0], rsr.at[z_peer(i)], rs_out.at[i], rs_sem.at[z_peer(i)], (x, z, h)
        ).wait_recv()
    acc = rsr[0].astype(F32)
    for i in range(1, nz):
        acc = acc + rsr[i].astype(F32)
    xs[...] = acc.astype(BF16)
    for i in range(1, nx):
        copy = put(xs, xr.at[x], x_out.at[i], x_sem.at[x], (x_peer(i), z, h))
        copy.start()
        sent.append(copy)
    xr[x] = xs[...]
    for i in range(1, nx):
        put(
            xs, xr.at[x_peer(i)], x_out.at[i], x_sem.at[x_peer(i)], (x, z, h)
        ).wait_recv()
    acc = xr[0].astype(F32)
    for i in range(1, nx):
        acc = acc + xr[i].astype(F32)
    wf[z] = acc.astype(BF16)
    for i in range(1, nz):
        copy = put(
            wf.at[z], wf.at[z], wf_out.at[i], wf_sem.at[z], (x, z_peer(i), h)
        )
        copy.start()
        sent.append(copy)
    for i in range(1, nz):
        put(
            wf.at[z], wf.at[z_peer(i)], wf_out.at[i], wf_sem.at[z_peer(i)], (x, z, h)
        ).wait_recv()
    for j in range(nz):
        tile = wf[j].astype(F32)
        gdw_ref[:, j * piece : (j + 1) * piece] = tile[:heads]
        gww_ref[:, j * piece : (j + 1) * piece] = tile[heads:]

    for copy in sent:
        copy.wait_send()

    @pl.when(b > 0)
    def _():
        for i in every:
            put(m1s.at[i], m1r.at[i], m1_out.at[i], m1_sem.at[i], (x, z, h)).wait_send()

    @pl.when(b == 0)
    def _():
        @pl.when(a > 0)
        def _():
            for i in every:
                put(
                    m2s.at[i], m2r.at[i], m2_out.at[i], m2_sem.at[i], (x, z, h)
                ).wait_send()

        @pl.when(a == 0)
        def _():
            @pl.when(x > 0)
            def _():
                for i in every:
                    put(fs.at[i], fr.at[i], f_out.at[i], f_sem.at[i], (x, z, h)).wait_send()

            for i in every:
                for j in range(1, na):
                    put(
                        fr.at[i], fr.at[i], d_out.at[i, j], f_sem.at[i], (x, z, h)
                    ).wait_send()

        for i in every:
            for j in range(1, nb):
                put(
                    gr.at[i], gr.at[i], gr_out.at[i, j], gr_sem.at[i], (x, z, h)
                ).wait_send()


def shards(sizes, axes, q, k, v, dy, hid, wd, ww, dbias, dlog, wbias, s0):
    nx, na, nb, nh = sizes
    nz = na * nb
    n, heads, dk = q.shape
    depth = hid.shape[1]
    rows, flat = 2 * heads, (n * heads, dk)
    width, piece = depth // nh, depth // nz
    vmem = pl.BlockSpec(memory_space=pltpu.VMEM)
    smem = pl.BlockSpec(memory_space=pltpu.SMEM)
    dma = pltpu.SemaphoreType.DMA
    maps = pltpu.VMEM((heads, 2, dk, dk), BF16)
    ends = pltpu.VMEM((heads, dk, dk), BF16)
    out = pl.pallas_call(
        functools.partial(kernel, sizes, axes),
        out_shape=(
            jax.ShapeDtypeStruct(flat, BF16),
            jax.ShapeDtypeStruct(flat, BF16),
            jax.ShapeDtypeStruct(flat, BF16),
            jax.ShapeDtypeStruct((n, width), BF16),
            jax.ShapeDtypeStruct((heads, depth), F32),
            jax.ShapeDtypeStruct((heads, depth), F32),
        ),
        in_specs=[vmem] * 8 + [smem] * 3,
        out_specs=[vmem] * 6,
        scratch_shapes=[
            pltpu.VMEM(flat, F32), pltpu.VMEM(flat, F32),
            pltpu.VMEM(flat, F32), pltpu.VMEM(flat, F32),
            pltpu.VMEM((rows, depth), BF16),
            pltpu.VMEM((nh, rows, width), BF16),
            pltpu.VMEM((nh, rows, n), BF16),
            pltpu.VMEM((nz, rows, n), F32),
            pltpu.VMEM((heads, dk, dk), F32), pltpu.VMEM((heads, dk, dk), F32),
            maps, maps, maps, maps, ends, ends, ends,
            pltpu.VMEM((nz, rows, piece), BF16), pltpu.VMEM((nz, rows, piece), BF16),
            pltpu.VMEM((rows, piece), BF16), pltpu.VMEM((nx, rows, piece), BF16),
            pltpu.VMEM((nz, rows, piece), BF16),
            dma((nh,)), dma((nh,)), dma((nz,)), dma((heads,)), dma((heads,)),
            dma((heads,)), dma((heads,)), dma((nz,)), dma((nx,)), dma((nz,)),
            dma((nh,)), dma((nh,)), dma((nz,)), dma((heads,)), dma((heads,)),
            dma((heads,)), dma((heads, na)), dma((heads, nb)),
            dma((nz,)), dma((nx,)), dma((nz,)),
        ],
        compiler_params=pltpu.CompilerParams(
            collective_id=0, has_side_effects=True, vmem_limit_bytes=48 * 2**20
        ),
    )(
        q.reshape(flat), k.reshape(flat), v.reshape(flat), dy.reshape(flat),
        hid, wd.T, ww.T, s0[0], dbias, dlog, wbias,
    )
    gq, gk, gv, gh, gdw, gww = out
    return (
        gq.reshape(q.shape), gk.reshape(q.shape), gv.reshape(q.shape),
        gh, gdw.T, gww.T,
    )


def solution(mesh):
    return build(mesh, (4, 4, 4))


def build(mesh, split):
    nx, na, nb = split
    nh = mesh.shape["head"]
    torus = Mesh(mesh.devices.reshape(nx, na * nb, nh), ("x", "z", "head"))
    seq = ("x", "z")
    by_head = P(seq, "head", None)
    in_specs = (
        by_head, by_head, by_head, by_head, P(seq, None),
        P(None, "head"), P(None, "head"), P("head"), P("head"), P("head"),
        P(seq, "head", None, None),
    )
    out_specs = (
        by_head, by_head, by_head, P(seq, "head"), P(None, "head"), P(None, "head"),
    )
    return jax.shard_map(
        functools.partial(shards, (nx, na, nb, nh), ("x", "z", "head")),
        mesh=torus, in_specs=in_specs, out_specs=out_specs, check_vma=False,
    )
```
